32 devices in a mesh: gx: 2 (over y), gy: 4 (over z), gz: 4 (over x, core).
Axes of the slice: x: 2, y: 2, z: 4, core: 2. Of those that a mesh axis runs over, the one named last changes fastest.
Arguments:
- positions: float32 [2, 4, 4, 3, 48], P('gx', 'gy', 'gz'), may hold values from 0 to 1
- species: int32 [2, 4, 4, 48], P('gx', 'gy', 'gz'), may hold values from 0 to 3
- neighbours: int32 [2, 4, 4, 48, 128], P('gx', 'gy', 'gz'), may hold values from 0 to 1295
- neigh_counts: int32 [2, 4, 4, 48], P('gx', 'gy', 'gz'), may hold values from 64 to 128
- embedding: bfloat16 [4, 128], replicated, may hold values from -6 to 6
- rbf_decay: float32 [16], replicated, may hold values from 0.2 to 5
- radial_weight: bfloat16 [2, 16, 128], replicated, may hold values from -1.5 to 1.5
- node_weight: bfloat16 [2, 128, 128], replicated, may hold values from -0.5 to 0.5
- readout: bfloat16 [128], replicated, may hold values from -0.5 to 0.5
- species_bias: float32 [4], replicated, may hold values from -4 to 4
Outputs:
- atom_energy: float32 [2, 4, 4, 48], P('gx', 'gy', 'gz')
- total_energy: float32 [], replicated
The draws below stay inside these ranges and needn't reach their ends.
Inputs may be any that keep to these rules, and one draw needn't show every extreme that they name: `neighbours`: the offset code of an entry is 9 (dx + 1) + 3 (dy + 1) + (dz + 1) for a cell offset of -1, 0 or 1 along each dimension.
All inputs are finite; a program needn't handle non-finite values.
Results may differ from the reference program's by a relative error of at most 0.0028.
Values may be sent and summed in bfloat16 or wider, within the bound.
A program may use at most 64 MiB of HBM per device.

```python
import math
import jax
import jax.numpy as jnp
from jax import lax

F = 128
NB = 128
NRBF = 16
NSPEC = 4
SLOTS = 48
LAYERS = 2
NX = 2
NY = 4
NZ = 4


def plant(result, key, least, largest):
    extent = result.shape
    spot = [jax.random.randint(jax.random.fold_in(key, axis), (), 0, extent[axis]) for axis in range(len(extent))]
    result = result.at[tuple(spot)].set(least)
    longest = extent.index(max(extent))
    spot[longest] = (spot[longest] + 1) % extent[longest]
    return result.at[tuple(spot)].set(largest)


def block_levels(rng, shape, cuts, smallest, top_value):
    loudness = 1.0
    for dim, blocks in cuts:
        draws = jax.random.uniform(jax.random.fold_in(jax.random.fold_in(rng, 6), dim), (blocks,), jnp.float32, smallest / len(cuts), top_value / len(cuts))
        loudness = loudness * jnp.repeat(jnp.exp(draws), shape[dim] // blocks).reshape((-1,) + (1,) * (len(shape) - 1 - dim))
    return loudness


def bell_draw(stream_key, shape, spread, most, kind=jnp.bfloat16):
    entries = spread * jax.random.normal(stream_key, shape, jnp.float32)
    return jnp.clip(entries, min=-most, max=most).astype(kind)


def setup_inputs(seed: int = 0) -> dict:
    splits = jax.random.split(jax.random.key(seed), 11)
    return {
        "positions": jnp.clip(1.0 * jax.random.uniform(splits[0], (NX, NY, NZ, 3, SLOTS), jnp.float32) ** block_levels(splits[0], (NX, NY, NZ, 3, SLOTS), ((0, 2), (1, 4), (2, 4)), -0.2, 0.2), 0.0, 1.0),
        "species": plant(jax.random.randint(splits[1], (NX, NY, NZ, SLOTS), 0, NSPEC), jax.random.fold_in(splits[1], 1), 0, NSPEC - 1).astype(jnp.int32),
        "neighbours": plant(jax.random.randint(splits[2], (NX, NY, NZ, SLOTS, NB), 0, 27 * SLOTS), jax.random.fold_in(splits[2], 1), 0, (27 * SLOTS) - 1).astype(jnp.int32),
        "neigh_counts": plant(jax.random.randint(splits[3], (NX, NY, NZ, SLOTS), NB // 2, NB + 1), jax.random.fold_in(splits[3], 1), NB // 2, NB).astype(jnp.int32),
        "embedding": bell_draw(splits[4], (NSPEC, F), 1.0, 6.0),
        "rbf_decay": jnp.clip(jnp.exp(jax.random.uniform(splits[5], (NRBF,), jnp.float32, math.log(0.2), math.log(5.0))), 0.2, 5.0),
        "radial_weight": bell_draw(splits[6], (LAYERS, NRBF, F), NRBF ** -0.5, 1.5),
        "node_weight": bell_draw(splits[7], (LAYERS, F, F), F ** -0.5, 0.5),
        "readout": bell_draw(splits[8], (F,), F ** -0.5, 0.5),
        "species_bias": bell_draw(splits[9], (NSPEC,), 1.0, 4.0, jnp.float32),
    }


def embed_atoms(species, embedding):
    kind_count = embedding.shape[0]
    one_hot = (species[..., None] == jnp.arange(kind_count, dtype=jnp.int32)).astype(jnp.bfloat16)
    embedded = jnp.dot(one_hot.reshape(-1, kind_count), embedding, preferred_element_type=jnp.float32)
    return embedded.astype(jnp.bfloat16).reshape(species.shape + (embedding.shape[1],))

def interaction(hidden_slab, place_slab, neighbour_row, count_row, rbf_decay, radial_weight, node_weight):
    cell_count, slot_count, neighbour_count = neighbour_row.shape
    feature_width = hidden_slab.shape[-1]
    slab_depth = cell_count + 2
    code_offset = neighbour_row // slot_count
    slot_index = neighbour_row % slot_count
    shift_x = code_offset // 9
    shift_y = code_offset // 3 % 3
    shift_z = code_offset % 3
    cell_column = lax.broadcasted_iota(jnp.int32, neighbour_row.shape, 0)
    cell_index = ((shift_x * 3 + shift_y) * slab_depth + cell_column + shift_z).reshape(-1)
    slot_flat = slot_index.reshape(-1)
    neighbour_feats = jnp.take(hidden_slab.reshape(-1, feature_width), cell_index * slot_count + slot_flat, axis=0)
    place_flat = place_slab.reshape(9 * slab_depth, 3, slot_count)
    far_place = place_flat[cell_index, :, slot_flat]
    centre = jnp.transpose(place_slab[1, 1, 1:slab_depth - 1], (0, 2, 1))
    offsets_xyz = jnp.stack([shift_x - 1, shift_y - 1, shift_z - 1], axis=-1).astype(jnp.float32)
    displace = far_place.reshape(cell_count, slot_count, neighbour_count, 3) + offsets_xyz - centre[:, :, None, :]
    distance_sq = lax.optimization_barrier(jnp.sum(displace * displace, axis=-1))
    radial_basis = jnp.exp(-distance_sq[..., None] * rbf_decay).astype(jnp.bfloat16).reshape(-1, rbf_decay.shape[0])
    filters = jnp.dot(radial_basis, radial_weight, preferred_element_type=jnp.float32)
    live_mask = (lax.broadcasted_iota(jnp.int32, neighbour_row.shape, 2) < count_row[:, :, None]).reshape(-1, 1)
    terms = jnp.where(live_mask, filters * neighbour_feats.astype(jnp.float32), jnp.float32(0.0))
    message = terms.reshape(cell_count * slot_count, neighbour_count, feature_width).sum(axis=1)
    inv_scale = lax.rsqrt(lax.optimization_barrier(jnp.mean(message * message, axis=-1, keepdims=True)) + 1e-05)
    normed = (message * inv_scale).astype(jnp.bfloat16)
    update = jax.nn.silu(jnp.dot(normed, node_weight, preferred_element_type=jnp.float32))
    own_rows = hidden_slab[1, 1, 1:slab_depth - 1].reshape(-1, feature_width).astype(jnp.float32)
    return (own_rows + update).astype(jnp.bfloat16).reshape(cell_count, slot_count, feature_width)

def run_layer(hidden_pad, place_pad, neighbours, neigh_counts, rbf_decay, radial_weight, node_weight):
    span_x = neighbours.shape[0]
    span_y = neighbours.shape[1]

    def one_row(row_index):
        row_x = row_index // span_y
        row_y = row_index % span_y
        hidden_slab = lax.dynamic_slice_in_dim(lax.dynamic_slice_in_dim(hidden_pad, row_x, 3, 0), row_y, 3, 1)
        place_slab = lax.dynamic_slice_in_dim(lax.dynamic_slice_in_dim(place_pad, row_x, 3, 0), row_y, 3, 1)
        return interaction(hidden_slab, place_slab, neighbours[row_x, row_y], neigh_counts[row_x, row_y], rbf_decay, radial_weight, node_weight)
    row_results = lax.map(one_row, jnp.arange(span_x * span_y, dtype=jnp.int32))
    return row_results.reshape((span_x, span_y) + row_results.shape[1:])

def atom_energies(hidden, species, readout, species_bias):
    per_atom = lax.optimization_barrier(jnp.sum(hidden.astype(jnp.float32) * readout.astype(jnp.float32), axis=-1))
    one_hot = (species[..., None] == jnp.arange(species_bias.shape[0], dtype=jnp.int32)).astype(jnp.float32)
    return per_atom + lax.optimization_barrier(jnp.sum(one_hot * species_bias, axis=-1))

def reference(positions, species, neighbours, neigh_counts, embedding, rbf_decay, radial_weight, node_weight, readout, species_bias):
    pad_spec = ((1, 1), (1, 1), (1, 1), (0, 0), (0, 0))
    place_pad = jnp.pad(positions, pad_spec, mode='wrap')
    hidden = embed_atoms(species, embedding)
    for layer_index in range(LAYERS):
        hidden_pad = jnp.pad(hidden, pad_spec, mode='wrap')
        hidden = run_layer(hidden_pad, place_pad, neighbours, neigh_counts, rbf_decay, radial_weight[layer_index], node_weight[layer_index])
    energy = atom_energies(hidden, species, readout, species_bias)
    return (energy, jnp.sum(energy))
```

```python
import functools
import itertools
import math

import jax
import jax.numpy as jnp
from jax import lax
from jax.experimental import pallas as pl
from jax.experimental.pallas import tpu as pltpu
from jax.sharding import PartitionSpec as P

AXES = ("gx", "gy", "gz")
MESH = pl.DeviceIdType.MESH
LANES = 128
LOG2E = math.log2(math.e)


def distinct(count):
    return (0,) if count == 1 else (0, -1) if count == 2 else (0, -1, 1)


def canonical(offset, count):
    return 0 if count == 1 else -abs(offset) if count == 2 else offset


def round_up(value, unit):
    return -(-value // unit) * unit


def reach(sizes, steps):
    found = {(0, 0, 0)}
    for _ in range(steps):
        found = {
            tuple((a + b) % n for a, b, n in zip(shift, off, sizes))
            for shift in found
            for off in itertools.product((-1, 0, 1), repeat=3)
        }
    return found


def kernel(
    sizes,
    stages,
    pos_any,
    spec_any,
    nbr_any,
    cnt_any,
    emb_any,
    decay_any,
    radial_any,
    node_any,
    readout_any,
    bias_any,
    out_ref,
    places,
    cols,
    hist,
    codes,
    basis,
    feats0,
    feats1,
    *rest,
):
    anys = (
        pos_any, spec_any, nbr_any, cnt_any, emb_any, decay_any, radial_any, node_any, readout_any, bias_any,
    )
    pos_ref, spec_ref, nbr_ref, cnt_ref, emb_ref = rest[:5]
    decay_ref, radial_ref, node_ref, readout_ref, bias_ref = rest[5:10]
    local = rest[:10]
    load_sem = rest[10]
    rest = rest[11:]
    stage_bufs = rest[: len(stages)]
    pos_send, pos_recv, hid_send, hid_recv, red_send, red_recv = rest[len(stages) :]
    me = tuple(lax.axis_index(name) for name in AXES)
    slots = pos_any.shape[-1]
    neighbour_count = nbr_any.shape[-1]
    features = emb_any.shape[1]
    kinds = emb_any.shape[0]
    basis_count = radial_ref.shape[1]
    hi_rows = hist.shape[0] // slots
    block = 9 * slots
    far_base = round_up(2 * block, LANES)
    columns = basis.shape[1]
    xd, yd, zd = (distinct(n) for n in sizes)
    group = len(xd) * len(zd)
    split = len(yd) == 3

    loads = [
        pltpu.make_async_copy(src, dst, load_sem.at[n])
        for n, (src, dst) in enumerate(zip(anys, local))
    ]
    for n in (0, 1, 3, 2, 4, 5, 6, 7, 8, 9):
        loads[n].start()

    def wrapped(coord, delta, count):
        if isinstance(delta, int):
            return lax.rem(coord + (delta % count), count) if delta % count else coord
        return lax.rem(coord + delta + count, count)

    def device(shift):
        return tuple(wrapped(c, d, n) for c, d, n in zip(me, shift, sizes))

    def last_offset(coord):
        return jnp.where(2 * coord < sizes[1], -1, 1)

    side = last_offset(me[1])

    neighbours = [off for off in itertools.product(xd, yd, zd) if off != (0, 0, 0)]
    stage_shifts = [
        [
            shift
            for shift in itertools.product(
                *(range(n) if name in axes else (0,) for name, n in zip(AXES, sizes))
            )
            if any(shift)
        ]
        for axes in stages
    ]
    known = reach(sizes, 2)
    partners = {tuple((-d) % n for d, n in zip(off, sizes)) for off in neighbours}
    for shifts in stage_shifts:
        partners.update(shift for shift in shifts if shift not in known)
    barrier = pltpu.get_barrier_semaphore()
    for shift in sorted(partners):
        pl.semaphore_signal(barrier, inc=1, device_id=device(shift), device_id_type=MESH)

    def ordered_sends():
        planes = sorted(
            itertools.product(xd, zd), key=lambda o: -(abs(o[0]) + abs(o[1]))
        )
        ways = (-side, side, 0) if split else yd[::-1]
        return [
            (xo, yo, zo)
            for yo in ways
            for xo, zo in planes
            if not (isinstance(yo, int) and (xo, yo, zo) == (0, 0, 0))
        ]

    def group_of(yo):
        if isinstance(yo, int):
            return 0 if yo == 0 else 1
        return jnp.where(yo == last_offset(wrapped(me[1], -yo, sizes[1])), 2, 1)

    def sem_of(yo):
        if isinstance(yo, int):
            return 0
        return group_of(yo) - 1

    loads[0].wait()
    loads[1].wait()
    places[0] = jnp.zeros(places.shape[1:], jnp.float32)
    places[0, 0:3, 0:slots] = pos_ref[0, 0, :, 0]
    places[0, 3:4, 0:slots] = spec_ref[0, 0].astype(jnp.float32)

    def prepare():
        loads[3].wait()
        counts = jnp.concatenate(
            [cnt_ref[0, 0].astype(jnp.float32), jnp.zeros((1, LANES - slots), jnp.float32)], axis=1
        )
        turned = jnp.transpose(
            jnp.concatenate([places[0], counts, jnp.zeros((3, LANES), jnp.float32)], axis=0)
        )[0:slots]
        cols[:, 0:8] = turned
        count_col = turned[:, 4:5]
        loads[2].wait()
        raw = nbr_ref[0, 0, 0]
        live = lax.broadcasted_iota(jnp.int32, raw.shape, 1).astype(jnp.float32) < count_col
        x_step = jnp.where(raw >= 2 * block, 2, jnp.where(raw >= block, 1, 0))
        inner = raw - x_step * block
        y_low = inner < 3 * slots
        y_high = inner >= 6 * slots
        depth = inner - jnp.where(y_low, 0, jnp.where(y_high, 6 * slots, 3 * slots))
        low_base = jnp.where(side < 0, far_base, block)
        high_base = jnp.where(side < 0, block, far_base)
        place = depth + x_step * (3 * slots) + jnp.where(
            y_low, low_base, jnp.where(y_high, high_base, 0)
        )
        codes[...] = jnp.where(live, place, hi_rows * LANES - 1)
        hi_iota = lax.broadcasted_iota(jnp.int32, (hi_rows, neighbour_count), 0)
        lo_iota = lax.broadcasted_iota(jnp.int32, (LANES, neighbour_count), 0)
        for atom in range(slots):
            row = codes[atom : atom + 1, :]
            high = jnp.where((row >> 7) == hi_iota, 1.0, 0.0).astype(jnp.bfloat16)
            low = jnp.where((row & (LANES - 1)) == lo_iota, 1.0, 0.0).astype(jnp.bfloat16)
            hist[atom * hi_rows : (atom + 1) * hi_rows, :] = lax.dot_general(
                high, low, (((1,), (1,)), ((), ())), preferred_element_type=jnp.float32
            )

    early = side < 0
    pl.when(early)(prepare)
    pl.semaphore_wait(barrier, len(partners))

    def slot_of(xo, yo, zo):
        return group_of(yo) * group + xd.index(xo) * len(zd) + zd.index(zo)

    place_copies = [
        pltpu.make_async_remote_copy(
            src_ref=places.at[0],
            dst_ref=places.at[slot_of(*off)],
            send_sem=pos_send.at[0],
            recv_sem=pos_recv.at[sem_of(off[1])],
            device_id=device(tuple(-d for d in off)),
            device_id_type=MESH,
        )
        for off in ordered_sends()
    ]
    for copy in place_copies:
        copy.start()
    pl.when(jnp.logical_not(early))(prepare)

    for n in range(4, 10):
        loads[n].wait()
    near_rows = slice(2 * block, far_base)
    far_rows = slice(far_base + block, columns)
    for span in (near_rows, far_rows):
        if span.stop > span.start:
            feats1[span, :] = jnp.zeros((span.stop - span.start, features), jnp.bfloat16)
    own_pos = [jnp.broadcast_to(cols[:, c : c + 1], (slots, LANES)) for c in range(3)]
    species_col = cols[:, 3:4]
    own_hidden = jnp.zeros((slots, features), jnp.float32)
    for kind in range(kinds):
        own_hidden = jnp.where(
            species_col == float(kind), emb_ref[kind : kind + 1, :].astype(jnp.float32), own_hidden
        )
    emb = emb_ref[...].astype(jnp.float32)
    if kinds < 8:
        emb = jnp.concatenate([emb, jnp.zeros((8 - kinds, features), jnp.float32)], axis=0)
    emb = emb.astype(jnp.bfloat16)
    scales = [decay_ref[b] * (-LOG2E) for b in range(basis_count)]
    lane4 = lax.broadcasted_iota(jnp.int32, (4, LANES), 1)
    sub4 = lax.broadcasted_iota(jnp.int32, (4, LANES), 0)
    sub = lax.broadcasted_iota(jnp.int32, (8, LANES), 0)

    phases = (
        ([(0, 0), (1, -side)], 0, far_base),
        ([(2, side)], far_base, columns),
    )

    def source_slot(row, dx, dz):
        if not split:
            row = 0 if row == 0 or sizes[1] == 1 else 1
        x = xd.index(canonical(dx, sizes[0]))
        z = zd.index(canonical(dz, sizes[2]))
        return row * group + x * len(zd) + z

    def tables(phase):
        rows, first, stop = phases[phase]
        flat = [jnp.zeros((4, LANES), jnp.float32) for _ in range((stop - first) // LANES)]
        column = 0
        for row, dy in rows:
            for dx, dz in itertools.product((-1, 0, 1), repeat=2):
                cell = places[source_slot(row, dx, dz)]
                delta = jnp.zeros((4, LANES), jnp.float32)
                if dx:
                    delta = jnp.where(sub4 == 0, float(dx), delta)
                if row:
                    delta = jnp.where(sub4 == 1, jnp.asarray(dy, jnp.float32), delta)
                if dz:
                    delta = jnp.where(sub4 == 2, float(dz), delta)
                if dx or row or dz:
                    cell = cell + delta
                tile, start = divmod(column, LANES)
                if start:
                    cell = pltpu.roll(cell, start, 1)
                end = start + slots
                flat[tile] = jnp.where((lane4 >= start) & (lane4 < end), cell, flat[tile])
                if end > LANES:
                    flat[tile + 1] = jnp.where(lane4 < end - LANES, cell, flat[tile + 1])
                column += slots
        for index, table in enumerate(flat):
            span = slice(first + index * LANES, first + (index + 1) * LANES)
            r2 = jnp.zeros((slots, LANES), jnp.float32)
            for c in range(3):
                delta = table[c : c + 1, :] - own_pos[c]
                r2 = r2 + delta * delta
            times = hist[pl.ds(first // LANES + index, slots, stride=hi_rows), :]
            for b in range(basis_count):
                basis[b * slots : (b + 1) * slots, span] = (
                    jnp.exp2(r2 * scales[b]) * times
                ).astype(jnp.bfloat16)
            one_hot = jnp.where(table[3:4, :].astype(jnp.int32) == sub, 1.0, 0.0)
            feats0[span, :] = jnp.dot(
                jnp.transpose(one_hot).astype(jnp.bfloat16), emb, preferred_element_type=jnp.float32
            ).astype(jnp.bfloat16)

    def gather(layer, feats, phase, message):
        _, first, stop = phases[phase]
        weight = radial_ref[layer].astype(jnp.float32)
        step = basis_count // 4
        for lead_b in range(0, basis_count, step):
            collected = jnp.dot(
                basis[lead_b * slots : (lead_b + step) * slots, first:stop],
                feats[first:stop, :],
                preferred_element_type=jnp.float32,
            )
            for b in range(step):
                message = message + (
                    collected[b * slots : (b + 1) * slots] * weight[lead_b + b : lead_b + b + 1]
                )
        return message

    def update(layer, message, hidden):
        inv_scale = lax.rsqrt(jnp.mean(message * message, axis=-1, keepdims=True) + 1e-05)
        normed = (message * inv_scale).astype(jnp.bfloat16)
        value = jnp.dot(normed, node_ref[layer], preferred_element_type=jnp.float32)
        return (hidden + value / (1.0 + jnp.exp(-value))).astype(jnp.bfloat16)

    def landed(ref, sem):
        pltpu.make_async_copy(ref, ref, sem).wait()

    near_count = (2 if split else len(yd)) * group - 1
    far_count = group if split else 0

    message = jnp.zeros((slots, features), jnp.float32)
    if near_count:
        landed(places.at[pl.ds(0, near_count)], pos_recv.at[0])
    tables(0)
    message = gather(0, feats0, 0, message)
    if far_count:
        landed(places.at[pl.ds(0, far_count)], pos_recv.at[1])
    tables(1)
    message = gather(0, feats0, 1, message)
    hidden1 = update(0, message, own_hidden)

    def row_of(base, dx, dz):
        return base + (3 * (dx + 1) + dz + 1) * slots

    own_rows = pl.ds(row_of(0, 0, 0), slots)
    feats1[own_rows, :] = hidden1

    def target_base(yo):
        if isinstance(yo, int):
            return 0 if yo == 0 else block
        return jnp.where(group_of(yo) == 2, far_base, block)

    hidden_copies = [
        pltpu.make_async_remote_copy(
            src_ref=feats1.at[own_rows],
            dst_ref=feats1.at[pl.ds(pl.multiple_of(row_of(target_base(off[1]), off[0], off[2]), 16), slots)],
            send_sem=hid_send.at[0],
            recv_sem=hid_recv.at[sem_of(off[1])],
            device_id=device(tuple(-d for d in off)),
            device_id_type=MESH,
        )
        for off in ordered_sends()
    ]
    for copy in hidden_copies:
        copy.start()

    species_row = places[0, 3:4, :]
    offsets = jnp.zeros((1, LANES), jnp.float32)
    for kind in range(kinds):
        offsets = jnp.where(species_row == float(kind), bias_ref[kind], offsets)
    offsets = jnp.where(lane4[0:1] < slots, offsets, 0.0)

    def spread(phase):
        for row, _ in phases[phase][0]:
            base = (0, block, far_base)[row]
            from_base = (0, block, block)[row] if not split else base
            if sizes[1] == 1:
                from_base = 0
            for dx, dz in itertools.product((-1, 0, 1), repeat=2):
                source = row_of(from_base, canonical(dx, sizes[0]), canonical(dz, sizes[2]))
                if source != row_of(base, dx, dz):
                    feats1[pl.ds(row_of(base, dx, dz), slots), :] = feats1[pl.ds(source, slots), :]

    message = jnp.zeros((slots, features), jnp.float32)
    if near_count:
        landed(feats1.at[pl.ds(0, near_count * slots)], hid_recv.at[0])
    spread(0)
    message = gather(1, feats1, 0, message)
    if far_count:
        landed(feats1.at[pl.ds(0, far_count * slots)], hid_recv.at[1])
    spread(1)
    message = gather(1, feats1, 1, message)
    hidden2 = update(1, message, hidden1.astype(jnp.float32))
    padded = jnp.concatenate(
        [hidden2, jnp.zeros((LANES - slots, features), jnp.bfloat16)], axis=0
    )
    readout = jnp.broadcast_to(readout_ref[...], (16, features))
    per_atom = lax.dot_general(
        readout, padded, (((1,), (1,)), ((), ())), preferred_element_type=jnp.float32
    )
    running = per_atom[0:1, :] + offsets
    energies = running

    for index, (axes, shifts, buf) in enumerate(zip(stages, stage_shifts, stage_bufs)):
        def rank_of(coords):
            rank = 0
            for name, coord, count in zip(AXES, coords, sizes):
                if name in axes:
                    rank = rank * count + coord
            return rank

        mine = rank_of(me)
        buf[mine] = running
        copies = [
            pltpu.make_async_remote_copy(
                src_ref=buf.at[mine],
                dst_ref=buf.at[mine],
                send_sem=red_send.at[index],
                recv_sem=red_recv.at[index],
                device_id=device(shift),
                device_id_type=MESH,
            )
            for shift in sorted(
                shifts, key=lambda s: -sum(min(d, n - d) for d, n in zip(s, sizes))
            )
        ]
        for copy in copies:
            copy.start()
        if copies:
            landed(buf.at[pl.ds(0, len(copies))], red_recv.at[index])
        running = jnp.sum(buf[...], axis=0)
    out_ref[0:1, :] = energies
    out_ref[1:2, :] = jnp.broadcast_to(jnp.sum(running, axis=1, keepdims=True), (1, LANES))
    if place_copies:
        landed(places.at[pl.ds(0, len(place_copies))], pos_send.at[0])
        landed(feats1.at[pl.ds(0, len(hidden_copies) * slots)], hid_send.at[0])
    for index, (shifts, buf) in enumerate(zip(stage_shifts, stage_bufs)):
        if shifts:
            landed(buf.at[pl.ds(0, len(shifts))], red_send.at[index])


def body(sizes, *args):
    positions, species, neighbours, _, embedding, decay, radial, _, readout, _ = args
    slots = positions.shape[-1]
    features = embedding.shape[1]
    basis_count = decay.shape[0]
    columns = round_up(18 * slots, LANES) + round_up(9 * slots, LANES)
    hi_rows = 16 * pl.cdiv(columns // LANES + 1, 16)
    devices = math.prod(sizes)
    stages = (AXES,) if devices <= 64 else tuple((name,) for name in AXES)
    stage_ranks = [
        math.prod(n for name, n in zip(AXES, sizes) if name in axes) for axes in stages
    ]
    cells = math.prod(len(distinct(n)) for n in sizes)
    vmem = pl.BlockSpec(memory_space=pltpu.VMEM)
    dma = pltpu.SemaphoreType.DMA
    operands = (
        jnp.transpose(positions, (0, 1, 3, 2, 4)),
        *args[1:8],
        readout.reshape(1, features),
        args[9],
    )
    scratch = [
        pltpu.VMEM((cells, 4, LANES), jnp.float32),
        pltpu.VMEM((slots, LANES), jnp.float32),
        pltpu.VMEM((slots * hi_rows, LANES), jnp.float32),
        pltpu.VMEM((slots, neighbours.shape[-1]), jnp.int32),
        pltpu.VMEM((basis_count * slots, columns), jnp.bfloat16),
        pltpu.VMEM((columns, features), jnp.bfloat16),
        pltpu.VMEM((columns, features), jnp.bfloat16),
    ]
    scratch += [
        pltpu.SMEM(x.shape, x.dtype)
        if x.ndim == 1
        else pltpu.VMEM(x.shape, x.dtype)
        for x in operands
    ] + [dma((len(operands),))]
    scratch += [pltpu.VMEM((count, 1, LANES), jnp.float32) for count in stage_ranks]
    scratch += [dma((1,)), dma((2,)), dma((1,)), dma((2,)), dma((len(stages),)), dma((len(stages),))]
    out = pl.pallas_call(
        functools.partial(kernel, sizes, stages),
        out_shape=pltpu.VMEM((2, LANES), jnp.float32),
        in_specs=[pl.BlockSpec(memory_space=pl.ANY)] * len(operands),
        out_specs=vmem,
        scratch_shapes=scratch,
        compiler_params=pltpu.CompilerParams(collective_id=0, has_side_effects=True),
    )(*operands)
    return out[0, :slots].reshape(species.shape), out[1, 0]


def solution(mesh):
    sizes = tuple(mesh.shape[name] for name in AXES)
    return jax.shard_map(
        functools.partial(body, sizes),
        mesh=mesh,
        in_specs=(
            P("gx", "gy", "gz", None, None),
            P("gx", "gy", "gz", None),
            P("gx", "gy", "gz", None, None),
            P("gx", "gy", "gz", None),
            P(),
            P(),
            P(),
            P(),
            P(),
            P(),
        ),
        out_specs=(P("gx", "gy", "gz", None), P()),
        check_vma=False,
    )
```

```python
import functools
import itertools
import math

import jax
import jax.numpy as jnp
from jax import lax
from jax.experimental import pallas as pl
from jax.experimental.pallas import tpu as pltpu
from jax.sharding import PartitionSpec as P

AXES = ("gx", "gy", "gz")
MESH = pl.DeviceIdType.MESH
LANES = 128
LOG2E = math.log2(math.e)


def distinct(count):
    return (0,) if count == 1 else (0, -1) if count == 2 else (0, -1, 1)


def canonical(offset, count):
    return 0 if count == 1 else -abs(offset) if count == 2 else offset


def is_set(offset):
    return not isinstance(offset, int) or offset != 0


def as_int(flag):
    return int(flag) if isinstance(flag, bool) else flag.astype(jnp.int32)


def round_up(value, unit):
    return -(-value // unit) * unit


def reach(sizes, steps):
    found = {(0, 0, 0)}
    for _ in range(steps):
        found = {
            tuple((a + b) % n for a, b, n in zip(shift, off, sizes))
            for shift in found
            for off in itertools.product((-1, 0, 1), repeat=3)
        }
    return found


def kernel(
    sizes,
    stages,
    pos_any,
    spec_any,
    nbr_any,
    cnt_any,
    emb_any,
    decay_any,
    radial_any,
    node_any,
    readout_any,
    bias_any,
    out_ref,
    places,
    cols,
    hist,
    codes,
    basis,
    feats0,
    feats1,
    *rest,
):
    anys = (
        pos_any, spec_any, nbr_any, cnt_any, emb_any, decay_any, radial_any, node_any, readout_any, bias_any,
    )
    pos_ref, spec_ref, nbr_ref, cnt_ref, emb_ref = rest[:5]
    decay_ref, radial_ref, node_ref, readout_ref, bias_ref = rest[5:10]
    local = rest[:10]
    load_sem = rest[10]
    rest = rest[11:]
    stage_bufs = rest[: len(stages)]
    pos_send, pos_recv, hid_send, hid_recv, red_send, red_recv, entered = rest[len(stages) :]
    me = tuple(lax.axis_index(name) for name in AXES)
    slots = pos_any.shape[-1]
    neighbour_count = nbr_any.shape[-1]
    features = emb_any.shape[1]
    kinds = emb_any.shape[0]
    basis_count = radial_ref.shape[1]
    hi_rows = hist.shape[0] // slots
    block = 9 * slots
    far_base = round_up(2 * block, LANES)
    columns = basis.shape[1]
    xd, yd, zd = (distinct(n) for n in sizes)
    group = len(xd) * len(zd)
    split = len(yd) == 3

    loads = [
        pltpu.make_async_copy(src, dst, load_sem.at[n])
        for n, (src, dst) in enumerate(zip(anys, local))
    ]
    for n in (0, 1, 3, 2, 4, 5, 6, 7, 8, 9):
        loads[n].start()

    def wrapped(coord, delta, count):
        if isinstance(delta, int):
            return lax.rem(coord + (delta % count), count) if delta % count else coord
        return lax.rem(coord + delta + count, count)

    def device(shift):
        return tuple(wrapped(c, d, n) for c, d, n in zip(me, shift, sizes))

    def last_offset(coord):
        return jnp.where(2 * coord < sizes[1], -1, 1)

    side = last_offset(me[1])

    stage_shifts = [
        [
            shift
            for shift in itertools.product(
                *(range(n) if name in axes else (0,) for name, n in zip(AXES, sizes))
            )
            if any(shift)
        ]
        for axes in stages
    ]
    def landed(ref, sem):
        pltpu.make_async_copy(ref, ref, sem).wait()

    far_z = jnp.where(lax.rem(me[2], 2) == 0, 1, -1) if len(zd) == 3 else zd[-1]
    ways_z = (far_z, -far_z, 0) if len(zd) == 3 else zd[::-1]
    ways_y = (-side, side) if split else yd[1:]

    def target(off):
        return tuple(wrapped(c, -d, n) for c, d, n in zip(me, off, sizes))

    ring = [(xo, 0, zo) for xo in xd[::-1] for zo in ways_z if is_set(xo) or is_set(zo)]
    across = [[(xo, yo, zo) for xo in xd[::-1] for zo in ways_z] for yo in ways_y]

    def wrap_of(yo):
        to = wrapped(me[1], -yo, sizes[1])
        return to - me[1] > 1, me[1] - to > 1

    known = reach(sizes, 2)
    others = sorted({s for shifts in stage_shifts for s in shifts if s not in known})
    barrier = pltpu.get_barrier_semaphore()

    for shift in others:
        pl.semaphore_signal(barrier, inc=1, device_id=device(shift), device_id_type=MESH)
    def greet(offs):
        for off in offs:
            pl.semaphore_signal(barrier, inc=1, device_id=target(off), device_id_type=MESH)

    greet(ring)
    greeted = len(ring) + len(others)
    for offs in across:
        low, high = wrap_of(offs[0][1])
        pl.when(jnp.logical_not(high))(functools.partial(greet, offs))
        greeted += len(offs) * (1 - as_int(low))

    def group_of(yo):
        if isinstance(yo, int):
            return 0 if yo == 0 else 1
        return jnp.where(yo == last_offset(wrapped(me[1], -yo, sizes[1])), 2, 1)

    def sem_of(yo):
        return group_of(yo)

    loads[0].wait()
    loads[1].wait()
    places[0] = jnp.zeros(places.shape[1:], jnp.float32)
    places[0, 0:3, 0:slots] = pos_ref[0, 0, :, 0]
    places[0, 3:4, 0:slots] = spec_ref[0, 0].astype(jnp.float32)

    def prepare():
        loads[3].wait()
        counts = jnp.concatenate(
            [cnt_ref[0, 0].astype(jnp.float32), jnp.zeros((1, LANES - slots), jnp.float32)], axis=1
        )
        turned = jnp.transpose(
            jnp.concatenate([places[0], counts, jnp.zeros((3, LANES), jnp.float32)], axis=0)
        )[0:slots]
        cols[:, 0:8] = turned
        count_col = turned[:, 4:5]
        loads[2].wait()
        raw = nbr_ref[0, 0, 0]
        live = lax.broadcasted_iota(jnp.int32, raw.shape, 1).astype(jnp.float32) < count_col
        x_step = jnp.where(raw >= 2 * block, 2, jnp.where(raw >= block, 1, 0))
        inner = raw - x_step * block
        y_low = inner < 3 * slots
        y_high = inner >= 6 * slots
        depth = inner - jnp.where(y_low, 0, jnp.where(y_high, 6 * slots, 3 * slots))
        low_base = jnp.where(side < 0, far_base, block)
        high_base = jnp.where(side < 0, block, far_base)
        place = depth + x_step * (3 * slots) + jnp.where(
            y_low, low_base, jnp.where(y_high, high_base, 0)
        )
        codes[...] = jnp.where(live, place, hi_rows * LANES - 1)
        hi_iota = lax.broadcasted_iota(jnp.int32, (hi_rows, neighbour_count), 0)
        lo_iota = lax.broadcasted_iota(jnp.int32, (LANES, neighbour_count), 0)
        for atom in range(slots):
            row = codes[atom : atom + 1, :]
            high = jnp.where((row >> 7) == hi_iota, 1.0, 0.0).astype(jnp.bfloat16)
            low = jnp.where((row & (LANES - 1)) == lo_iota, 1.0, 0.0).astype(jnp.bfloat16)
            hist[atom * hi_rows : (atom + 1) * hi_rows, :] = lax.dot_general(
                high, low, (((1,), (1,)), ((), ())), preferred_element_type=jnp.float32
            )

    def slot_of(xo, yo, zo):
        z = zd.index(zo) if isinstance(zo, int) else jnp.where(zo < 0, 1, 2)
        return group_of(yo) * group + xd.index(xo) * len(zd) + z

    def send_place(off):
        pltpu.make_async_remote_copy(
            src_ref=places.at[0],
            dst_ref=places.at[slot_of(*off)],
            send_sem=pos_send.at[0],
            recv_sem=pos_recv.at[sem_of(off[1])],
            device_id=target(off),
            device_id_type=MESH,
        ).start()

    early = side < 0
    pl.when(early)(prepare)
    pl.semaphore_wait(barrier, greeted)
    for offs in across:
        low, high = wrap_of(offs[0][1])

        @pl.when(high)
        def _():
            pl.semaphore_signal(
                entered, inc=1, device_id=target((0, offs[0][1], 0)), device_id_type=MESH
            )

    for off in ring:
        send_place(off)
    for offs in across:
        low, high = wrap_of(offs[0][1])

        @pl.when(jnp.logical_not(low))
        def _():
            for off in offs:
                send_place(off)

    pl.when(jnp.logical_not(early))(prepare)

    if group > 1:
        landed(places.at[pl.ds(0, group - 1)], pos_recv.at[0])
    for offs in across:
        low, high = wrap_of(offs[0][1])

        @pl.when(low)
        def _():
            yo = offs[0][1]
            pl.semaphore_wait(entered, 1)
            pltpu.make_async_remote_copy(
                src_ref=places.at[pl.ds(0, group)],
                dst_ref=places.at[pl.ds(group_of(yo) * group, group)],
                send_sem=pos_send.at[0],
                recv_sem=pos_recv.at[sem_of(yo)],
                device_id=target((0, yo, 0)),
                device_id_type=MESH,
            ).start()

    for n in range(4, 10):
        loads[n].wait()
    near_rows = slice(2 * block, far_base)
    far_rows = slice(far_base + block, columns)
    for span in (near_rows, far_rows):
        if span.stop > span.start:
            feats1[span, :] = jnp.zeros((span.stop - span.start, features), jnp.bfloat16)
    own_pos = [jnp.broadcast_to(cols[:, c : c + 1], (slots, LANES)) for c in range(3)]
    species_col = cols[:, 3:4]
    own_hidden = jnp.zeros((slots, features), jnp.float32)
    for kind in range(kinds):
        own_hidden = jnp.where(
            species_col == float(kind), emb_ref[kind : kind + 1, :].astype(jnp.float32), own_hidden
        )
    emb = emb_ref[...].astype(jnp.float32)
    if kinds < 8:
        emb = jnp.concatenate([emb, jnp.zeros((8 - kinds, features), jnp.float32)], axis=0)
    emb = emb.astype(jnp.bfloat16)
    scales = [decay_ref[b] * (-LOG2E) for b in range(basis_count)]
    lane4 = lax.broadcasted_iota(jnp.int32, (4, LANES), 1)
    sub4 = lax.broadcasted_iota(jnp.int32, (4, LANES), 0)
    sub = lax.broadcasted_iota(jnp.int32, (8, LANES), 0)

    phases = (
        ([(0, 0), (1, -side)], 0, far_base),
        ([(2, side)], far_base, columns),
    )

    def source_slot(row, dx, dz):
        if not split:
            row = 0 if row == 0 or sizes[1] == 1 else 1
        x = xd.index(canonical(dx, sizes[0]))
        z = zd.index(canonical(dz, sizes[2]))
        return row * group + x * len(zd) + z

    def tables(phase):
        rows, first, stop = phases[phase]
        flat = [jnp.zeros((4, LANES), jnp.float32) for _ in range((stop - first) // LANES)]
        column = 0
        for row, dy in rows:
            for dx, dz in itertools.product((-1, 0, 1), repeat=2):
                cell = places[source_slot(row, dx, dz)]
                delta = jnp.zeros((4, LANES), jnp.float32)
                if dx:
                    delta = jnp.where(sub4 == 0, float(dx), delta)
                if row:
                    delta = jnp.where(sub4 == 1, jnp.asarray(dy, jnp.float32), delta)
                if dz:
                    delta = jnp.where(sub4 == 2, float(dz), delta)
                if dx or row or dz:
                    cell = cell + delta
                tile, start = divmod(column, LANES)
                if start:
                    cell = pltpu.roll(cell, start, 1)
                end = start + slots
                flat[tile] = jnp.where((lane4 >= start) & (lane4 < end), cell, flat[tile])
                if end > LANES:
                    flat[tile + 1] = jnp.where(lane4 < end - LANES, cell, flat[tile + 1])
                column += slots
        for index, table in enumerate(flat):
            span = slice(first + index * LANES, first + (index + 1) * LANES)
            r2 = jnp.zeros((slots, LANES), jnp.float32)
            for c in range(3):
                delta = table[c : c + 1, :] - own_pos[c]
                r2 = r2 + delta * delta
            times = hist[pl.ds(first // LANES + index, slots, stride=hi_rows), :]
            for b in range(basis_count):
                basis[b * slots : (b + 1) * slots, span] = (
                    jnp.exp2(r2 * scales[b]) * times
                ).astype(jnp.bfloat16)
            one_hot = jnp.where(table[3:4, :].astype(jnp.int32) == sub, 1.0, 0.0)
            feats0[span, :] = jnp.dot(
                jnp.transpose(one_hot).astype(jnp.bfloat16), emb, preferred_element_type=jnp.float32
            ).astype(jnp.bfloat16)

    def gather(layer, feats, phase, message):
        _, first, stop = phases[phase]
        weight = radial_ref[layer].astype(jnp.float32)
        step = basis_count // 4
        for lead_b in range(0, basis_count, step):
            collected = jnp.dot(
                basis[lead_b * slots : (lead_b + step) * slots, first:stop],
                feats[first:stop, :],
                preferred_element_type=jnp.float32,
            )
            for b in range(step):
                message = message + (
                    collected[b * slots : (b + 1) * slots] * weight[lead_b + b : lead_b + b + 1]
                )
        return message

    def update(layer, message, hidden):
        inv_scale = lax.rsqrt(jnp.mean(message * message, axis=-1, keepdims=True) + 1e-05)
        normed = (message * inv_scale).astype(jnp.bfloat16)
        value = jnp.dot(normed, node_ref[layer], preferred_element_type=jnp.float32)
        return (hidden + value / (1.0 + jnp.exp(-value))).astype(jnp.bfloat16)

    group_rows = (group - 1,) + (group,) * len(ways_y)
    message = jnp.zeros((slots, features), jnp.float32)
    if len(ways_y) > 0:
        landed(places.at[pl.ds(0, group)], pos_recv.at[1])
    tables(0)
    message = gather(0, feats0, 0, message)
    if split:
        landed(places.at[pl.ds(0, group)], pos_recv.at[2])
    tables(1)
    message = gather(0, feats0, 1, message)
    hidden1 = update(0, message, own_hidden)

    def row_of(base, dx, dz):
        return base + (3 * (dx + 1) + dz + 1) * slots

    own_rows = pl.ds(row_of(0, 0, 0), slots)
    feats1[own_rows, :] = hidden1

    def target_base(yo):
        if isinstance(yo, int):
            return 0 if yo == 0 else block
        return jnp.where(group_of(yo) == 2, far_base, block)

    def send_hidden(offs):
        for off in offs:
            row = row_of(target_base(off[1]), off[0], off[2])
            pltpu.make_async_remote_copy(
                src_ref=feats1.at[own_rows],
                dst_ref=feats1.at[pl.ds(pl.multiple_of(row, 16), slots)],
                send_sem=hid_send.at[0],
                recv_sem=hid_recv.at[sem_of(off[1])],
                device_id=target(off),
                device_id_type=MESH,
            ).start()

    if split:
        upper = jnp.where(me[1] == 0, 1, -1)
        last = me[1] == sizes[1] - 1
        to_upper = [(xo, upper, zo) for xo in xd[::-1] for zo in ways_z]
        to_lower = [(xo, -upper, zo) for xo in xd[::-1] for zo in ways_z]
        pl.when(jnp.logical_not(last))(functools.partial(send_hidden, to_upper))
        send_hidden(ring)
        send_hidden(to_lower)
        pl.when(last)(functools.partial(send_hidden, to_upper))
    else:
        for offs in across + [ring]:
            send_hidden(offs)
    sent = len(ring) + sum(len(offs) for offs in across)

    species_row = places[0, 3:4, :]
    offsets = jnp.zeros((1, LANES), jnp.float32)
    for kind in range(kinds):
        offsets = jnp.where(species_row == float(kind), bias_ref[kind], offsets)
    offsets = jnp.where(lane4[0:1] < slots, offsets, 0.0)

    def spread(phase):
        for row, _ in phases[phase][0]:
            base = (0, block, far_base)[row]
            from_base = (0, block, block)[row] if not split else base
            if sizes[1] == 1:
                from_base = 0
            for dx, dz in itertools.product((-1, 0, 1), repeat=2):
                source = row_of(from_base, canonical(dx, sizes[0]), canonical(dz, sizes[2]))
                if source != row_of(base, dx, dz):
                    feats1[pl.ds(row_of(base, dx, dz), slots), :] = feats1[pl.ds(source, slots), :]

    message = jnp.zeros((slots, features), jnp.float32)
    for index, count in enumerate(group_rows[:2]):
        if count:
            landed(feats1.at[pl.ds(0, count * slots)], hid_recv.at[index])
    spread(0)
    message = gather(1, feats1, 0, message)
    if split:
        landed(feats1.at[pl.ds(0, group * slots)], hid_recv.at[2])
    spread(1)
    message = gather(1, feats1, 1, message)
    hidden2 = update(1, message, hidden1.astype(jnp.float32))
    padded = jnp.concatenate(
        [hidden2, jnp.zeros((LANES - slots, features), jnp.bfloat16)], axis=0
    )
    readout = jnp.broadcast_to(readout_ref[...], (16, features))
    per_atom = lax.dot_general(
        readout, padded, (((1,), (1,)), ((), ())), preferred_element_type=jnp.float32
    )
    running = per_atom[0:1, :] + offsets
    energies = running

    def ordered_shifts(axes):
        ys = (
            (side, *range(2, sizes[1] - 1), -side, 0) if split else tuple(range(sizes[1]))[::-1]
        )
        zs = (
            (-far_z, *range(2, sizes[2] - 1), far_z, 0)
            if len(zd) == 3
            else tuple(range(sizes[2]))[::-1]
        )
        xs = tuple(range(sizes[0]))[::-1]
        return [
            (x, y, z)
            for y in (ys if "gy" in axes else (0,))
            for x in (xs if "gx" in axes else (0,))
            for z in (zs if "gz" in axes else (0,))
            if is_set(x) or is_set(y) or is_set(z)
        ]

    for index, (axes, shifts, buf) in enumerate(zip(stages, stage_shifts, stage_bufs)):
        def rank_of(coords):
            rank = 0
            for name, coord, count in zip(AXES, coords, sizes):
                if name in axes:
                    rank = rank * count + coord
            return rank

        mine = rank_of(me)
        buf[mine] = running
        copies = [
            pltpu.make_async_remote_copy(
                src_ref=buf.at[mine],
                dst_ref=buf.at[mine],
                send_sem=red_send.at[index],
                recv_sem=red_recv.at[index],
                device_id=device(shift),
                device_id_type=MESH,
            )
            for shift in ordered_shifts(axes)
        ]
        for copy in copies:
            copy.start()
        if copies:
            landed(buf.at[pl.ds(0, len(copies))], red_recv.at[index])
        running = jnp.sum(buf[...], axis=0)
    out_ref[0:1, :] = energies
    out_ref[1:2, :] = jnp.broadcast_to(jnp.sum(running, axis=1, keepdims=True), (1, LANES))
    if sent:
        landed(places.at[pl.ds(0, sent)], pos_send.at[0])
        landed(feats1.at[pl.ds(0, sent * slots)], hid_send.at[0])
    for index, (shifts, buf) in enumerate(zip(stage_shifts, stage_bufs)):
        if shifts:
            landed(buf.at[pl.ds(0, len(shifts))], red_send.at[index])


def body(sizes, *args):
    positions, species, neighbours, _, embedding, decay, radial, _, readout, _ = args
    slots = positions.shape[-1]
    features = embedding.shape[1]
    basis_count = decay.shape[0]
    columns = round_up(18 * slots, LANES) + round_up(9 * slots, LANES)
    hi_rows = 16 * pl.cdiv(columns // LANES + 1, 16)
    devices = math.prod(sizes)
    stages = (AXES,) if devices <= 64 else tuple((name,) for name in AXES)
    stage_ranks = [
        math.prod(n for name, n in zip(AXES, sizes) if name in axes) for axes in stages
    ]
    cells = math.prod(len(distinct(n)) for n in sizes)
    vmem = pl.BlockSpec(memory_space=pltpu.VMEM)
    dma = pltpu.SemaphoreType.DMA
    operands = (
        jnp.transpose(positions, (0, 1, 3, 2, 4)),
        *args[1:8],
        readout.reshape(1, features),
        args[9],
    )
    scratch = [
        pltpu.VMEM((cells, 4, LANES), jnp.float32),
        pltpu.VMEM((slots, LANES), jnp.float32),
        pltpu.VMEM((slots * hi_rows, LANES), jnp.float32),
        pltpu.VMEM((slots, neighbours.shape[-1]), jnp.int32),
        pltpu.VMEM((basis_count * slots, columns), jnp.bfloat16),
        pltpu.VMEM((columns, features), jnp.bfloat16),
        pltpu.VMEM((columns, features), jnp.bfloat16),
    ]
    scratch += [
        pltpu.SMEM(x.shape, x.dtype)
        if x.ndim == 1
        else pltpu.VMEM(x.shape, x.dtype)
        for x in operands
    ] + [dma((len(operands),))]
    scratch += [pltpu.VMEM((count, 1, LANES), jnp.float32) for count in stage_ranks]
    scratch += [dma((1,)), dma((3,)), dma((1,)), dma((3,)), dma((len(stages),)), dma((len(stages),))]
    scratch += [pltpu.SemaphoreType.REGULAR]
    out = pl.pallas_call(
        functools.partial(kernel, sizes, stages),
        out_shape=pltpu.VMEM((2, LANES), jnp.float32),
        in_specs=[pl.BlockSpec(memory_space=pl.ANY)] * len(operands),
        out_specs=vmem,
        scratch_shapes=scratch,
        compiler_params=pltpu.CompilerParams(collective_id=0, has_side_effects=True),
    )(*operands)
    return out[0, :slots].reshape(species.shape), out[1, 0]


def solution(mesh):
    sizes = tuple(mesh.shape[name] for name in AXES)
    return jax.shard_map(
        functools.partial(body, sizes),
        mesh=mesh,
        in_specs=(
            P("gx", "gy", "gz", None, None),
            P("gx", "gy", "gz", None),
            P("gx", "gy", "gz", None, None),
            P("gx", "gy", "gz", None),
            P(),
            P(),
            P(),
            P(),
            P(),
            P(),
        ),
        out_specs=(P("gx", "gy", "gz", None), P()),
        check_vma=False,
    )
```

```python
import functools
import itertools
import math

import jax
import jax.numpy as jnp
from jax import lax
from jax.experimental import pallas as pl
from jax.experimental.pallas import tpu as pltpu
from jax.sharding import PartitionSpec as P

AXES = ("gx", "gy", "gz")
MESH = pl.DeviceIdType.MESH
LANES = 128
LOG2E = math.log2(math.e)


def distinct(count):
    return (0,) if count == 1 else (0, -1) if count == 2 else (0, -1, 1)


def canonical(offset, count):
    return 0 if count == 1 else -abs(offset) if count == 2 else offset


def is_set(offset):
    return not isinstance(offset, int) or offset != 0


def as_int(flag):
    return int(flag) if isinstance(flag, bool) else flag.astype(jnp.int32)


def round_up(value, unit):
    return -(-value // unit) * unit


def reach(sizes, steps):
    found = {(0, 0, 0)}
    for _ in range(steps):
        found = {
            tuple((a + b) % n for a, b, n in zip(shift, off, sizes))
            for shift in found
            for off in itertools.product((-1, 0, 1), repeat=3)
        }
    return found


def kernel(
    sizes,
    stages,
    pos_any,
    spec_any,
    nbr_any,
    cnt_any,
    emb_any,
    decay_any,
    radial_any,
    node_any,
    readout_any,
    bias_any,
    out_ref,
    places,
    cols,
    hist,
    codes,
    basis,
    feats0,
    feats1,
    *rest,
):
    anys = (
        pos_any, spec_any, nbr_any, cnt_any, emb_any, decay_any, radial_any, node_any, readout_any, bias_any,
    )
    pos_ref, spec_ref, nbr_ref, cnt_ref, emb_ref = rest[:5]
    decay_ref, radial_ref, node_ref, readout_ref, bias_ref = rest[5:10]
    local = rest[:10]
    load_sem = rest[10]
    rest = rest[11:]
    stage_bufs = rest[: len(stages)]
    pos_send, pos_recv, hid_send, hid_recv, red_send, red_recv, entered = rest[len(stages) :]
    me = tuple(lax.axis_index(name) for name in AXES)
    slots = pos_any.shape[-1]
    neighbour_count = nbr_any.shape[-1]
    features = emb_any.shape[1]
    kinds = emb_any.shape[0]
    basis_count = radial_ref.shape[1]
    hi_rows = hist.shape[0] // slots
    block = 9 * slots
    far_base = round_up(2 * block, LANES)
    columns = basis.shape[1]
    xd, yd, zd = (distinct(n) for n in sizes)
    group = len(xd) * len(zd)
    split = len(yd) == 3

    loads = [
        pltpu.make_async_copy(src, dst, load_sem.at[n])
        for n, (src, dst) in enumerate(zip(anys, local))
    ]
    for n in (0, 1, 3, 2, 4, 5, 6, 7, 8, 9):
        loads[n].start()

    def wrapped(coord, delta, count):
        if isinstance(delta, int):
            return lax.rem(coord + (delta % count), count) if delta % count else coord
        return lax.rem(coord + delta + count, count)

    def device(shift):
        return tuple(wrapped(c, d, n) for c, d, n in zip(me, shift, sizes))

    def last_offset(coord):
        return jnp.where(2 * coord < sizes[1], -1, 1)

    side = last_offset(me[1])

    stage_shifts = [
        [
            shift
            for shift in itertools.product(
                *(range(n) if name in axes else (0,) for name, n in zip(AXES, sizes))
            )
            if any(shift)
        ]
        for axes in stages
    ]
    def landed(ref, sem):
        pltpu.make_async_copy(ref, ref, sem).wait()

    far_z = jnp.where(lax.rem(me[2], 2) == 0, 1, -1) if len(zd) == 3 else zd[-1]
    ways_z = (far_z, -far_z, 0) if len(zd) == 3 else zd[::-1]
    ways_y = (-side, side) if split else yd[1:]

    def target(off):
        return tuple(wrapped(c, -d, n) for c, d, n in zip(me, off, sizes))

    ring = [(xo, 0, zo) for xo in xd[::-1] for zo in ways_z if is_set(xo) or is_set(zo)]
    across = [[(xo, yo, zo) for xo in xd[::-1] for zo in ways_z] for yo in ways_y]

    def wrap_of(yo):
        to = wrapped(me[1], -yo, sizes[1])
        return to - me[1] > 1, me[1] - to > 1

    known = reach(sizes, 2)
    others = sorted({s for shifts in stage_shifts for s in shifts if s not in known})
    barrier = pltpu.get_barrier_semaphore()

    for shift in others:
        pl.semaphore_signal(barrier, inc=1, device_id=device(shift), device_id_type=MESH)
    def greet(offs):
        for off in offs:
            pl.semaphore_signal(barrier, inc=1, device_id=target(off), device_id_type=MESH)

    greet(ring)
    greeted = len(ring) + len(others)
    for offs in across:
        low, high = wrap_of(offs[0][1])
        pl.when(jnp.logical_not(high))(functools.partial(greet, offs))
        greeted += len(offs) * (1 - as_int(low))

    def group_of(yo):
        if isinstance(yo, int):
            return 0 if yo == 0 else 1
        return jnp.where(yo == last_offset(wrapped(me[1], -yo, sizes[1])), 2, 1)

    def sem_of(yo):
        return group_of(yo)

    loads[0].wait()
    loads[1].wait()
    places[0] = jnp.zeros(places.shape[1:], jnp.float32)
    places[0, 0:3, 0:slots] = pos_ref[0, 0, :, 0]
    places[0, 3:4, 0:slots] = spec_ref[0, 0].astype(jnp.float32)

    def prepare():
        loads[3].wait()
        counts = jnp.concatenate(
            [cnt_ref[0, 0].astype(jnp.float32), jnp.zeros((1, LANES - slots), jnp.float32)], axis=1
        )
        turned = jnp.transpose(
            jnp.concatenate([places[0], counts, jnp.zeros((3, LANES), jnp.float32)], axis=0)
        )[0:slots]
        cols[:, 0:8] = turned
        count_col = turned[:, 4:5]
        loads[2].wait()
        raw = nbr_ref[0, 0, 0]
        live = lax.broadcasted_iota(jnp.int32, raw.shape, 1).astype(jnp.float32) < count_col
        x_step = jnp.where(raw >= 2 * block, 2, jnp.where(raw >= block, 1, 0))
        inner = raw - x_step * block
        y_low = inner < 3 * slots
        y_high = inner >= 6 * slots
        depth = inner - jnp.where(y_low, 0, jnp.where(y_high, 6 * slots, 3 * slots))
        low_base = jnp.where(side < 0, far_base, block)
        high_base = jnp.where(side < 0, block, far_base)
        place = depth + x_step * (3 * slots) + jnp.where(
            y_low, low_base, jnp.where(y_high, high_base, 0)
        )
        codes[...] = jnp.where(live, place, hi_rows * LANES - 1)
        hi_iota = lax.broadcasted_iota(jnp.int32, (hi_rows, neighbour_count), 0)
        lo_iota = lax.broadcasted_iota(jnp.int32, (LANES, neighbour_count), 0)
        for atom in range(slots):
            row = codes[atom : atom + 1, :]
            high = jnp.where((row >> 7) == hi_iota, 1.0, 0.0).astype(jnp.bfloat16)
            low = jnp.where((row & (LANES - 1)) == lo_iota, 1.0, 0.0).astype(jnp.bfloat16)
            hist[atom * hi_rows : (atom + 1) * hi_rows, :] = lax.dot_general(
                high, low, (((1,), (1,)), ((), ())), preferred_element_type=jnp.float32
            )

    def slot_of(xo, yo, zo):
        z = zd.index(zo) if isinstance(zo, int) else jnp.where(zo < 0, 1, 2)
        return group_of(yo) * group + xd.index(xo) * len(zd) + z

    def send_place(off):
        pltpu.make_async_remote_copy(
            src_ref=places.at[0],
            dst_ref=places.at[slot_of(*off)],
            send_sem=pos_send.at[0],
            recv_sem=pos_recv.at[sem_of(off[1])],
            device_id=target(off),
            device_id_type=MESH,
        ).start()

    early = side < 0
    pl.when(early)(prepare)
    pl.semaphore_wait(barrier, greeted)
    for offs in across:
        low, high = wrap_of(offs[0][1])

        @pl.when(high)
        def _():
            pl.semaphore_signal(
                entered, inc=1, device_id=target((0, offs[0][1], 0)), device_id_type=MESH
            )

    for off in ring:
        send_place(off)
    for offs in across:
        low, high = wrap_of(offs[0][1])

        @pl.when(jnp.logical_not(low))
        def _():
            for off in offs:
                send_place(off)

    pl.when(jnp.logical_not(early))(prepare)

    if group > 1:
        landed(places.at[pl.ds(0, group - 1)], pos_recv.at[0])
    for offs in across:
        low, high = wrap_of(offs[0][1])

        @pl.when(low)
        def _():
            yo = offs[0][1]
            pl.semaphore_wait(entered, 1)
            pltpu.make_async_remote_copy(
                src_ref=places.at[pl.ds(0, group)],
                dst_ref=places.at[pl.ds(group_of(yo) * group, group)],
                send_sem=pos_send.at[0],
                recv_sem=pos_recv.at[sem_of(yo)],
                device_id=target((0, yo, 0)),
                device_id_type=MESH,
            ).start()

    for n in range(4, 10):
        loads[n].wait()
    near_rows = slice(2 * block, far_base)
    far_rows = slice(far_base + block, columns)
    for span in (near_rows, far_rows):
        if span.stop > span.start:
            feats1[span, :] = jnp.zeros((span.stop - span.start, features), jnp.bfloat16)
    own_pos = [jnp.broadcast_to(cols[:, c : c + 1], (slots, LANES)) for c in range(3)]
    species_col = cols[:, 3:4]
    own_hidden = jnp.zeros((slots, features), jnp.float32)
    for kind in range(kinds):
        own_hidden = jnp.where(
            species_col == float(kind), emb_ref[kind : kind + 1, :].astype(jnp.float32), own_hidden
        )
    emb = emb_ref[...].astype(jnp.float32)
    if kinds < 8:
        emb = jnp.concatenate([emb, jnp.zeros((8 - kinds, features), jnp.float32)], axis=0)
    emb = emb.astype(jnp.bfloat16)
    scales = [decay_ref[b] * (-LOG2E) for b in range(basis_count)]
    lane4 = lax.broadcasted_iota(jnp.int32, (4, LANES), 1)
    sub4 = lax.broadcasted_iota(jnp.int32, (4, LANES), 0)
    sub = lax.broadcasted_iota(jnp.int32, (8, LANES), 0)

    phases = (
        ([(0, 0), (1, -side)], 0, far_base),
        ([(2, side)], far_base, columns),
    )

    def source_slot(row, dx, dz):
        if not split:
            row = 0 if row == 0 or sizes[1] == 1 else 1
        x = xd.index(canonical(dx, sizes[0]))
        z = zd.index(canonical(dz, sizes[2]))
        return row * group + x * len(zd) + z

    def tables(phase):
        rows, first, stop = phases[phase]
        flat = [jnp.zeros((4, LANES), jnp.float32) for _ in range((stop - first) // LANES)]
        column = 0
        for row, dy in rows:
            for dx, dz in itertools.product((-1, 0, 1), repeat=2):
                cell = places[source_slot(row, dx, dz)]
                delta = jnp.zeros((4, LANES), jnp.float32)
                if dx:
                    delta = jnp.where(sub4 == 0, float(dx), delta)
                if row:
                    delta = jnp.where(sub4 == 1, jnp.asarray(dy, jnp.float32), delta)
                if dz:
                    delta = jnp.where(sub4 == 2, float(dz), delta)
                if dx or row or dz:
                    cell = cell + delta
                tile, start = divmod(column, LANES)
                if start:
                    cell = pltpu.roll(cell, start, 1)
                end = start + slots
                flat[tile] = jnp.where((lane4 >= start) & (lane4 < end), cell, flat[tile])
                if end > LANES:
                    flat[tile + 1] = jnp.where(lane4 < end - LANES, cell, flat[tile + 1])
                column += slots
        for index, table in enumerate(flat):
            span = slice(first + index * LANES, first + (index + 1) * LANES)
            r2 = jnp.zeros((slots, LANES), jnp.float32)
            for c in range(3):
                delta = table[c : c + 1, :] - own_pos[c]
                r2 = r2 + delta * delta
            times = hist[pl.ds(first // LANES + index, slots, stride=hi_rows), :]
            for b in range(basis_count):
                basis[b * slots : (b + 1) * slots, span] = (
                    jnp.exp2(r2 * scales[b]) * times
                ).astype(jnp.bfloat16)
            one_hot = jnp.where(table[3:4, :].astype(jnp.int32) == sub, 1.0, 0.0)
            feats0[span, :] = jnp.dot(
                jnp.transpose(one_hot).astype(jnp.bfloat16), emb, preferred_element_type=jnp.float32
            ).astype(jnp.bfloat16)

    def gather(layer, feats, phase, message):
        _, first, stop = phases[phase]
        weight = radial_ref[layer].astype(jnp.float32)
        step = basis_count // 4
        for lead_b in range(0, basis_count, step):
            collected = jnp.dot(
                basis[lead_b * slots : (lead_b + step) * slots, first:stop],
                feats[first:stop, :],
                preferred_element_type=jnp.float32,
            )
            for b in range(step):
                message = message + (
                    collected[b * slots : (b + 1) * slots] * weight[lead_b + b : lead_b + b + 1]
                )
        return message

    def update(layer, message, hidden):
        inv_scale = lax.rsqrt(jnp.mean(message * message, axis=-1, keepdims=True) + 1e-05)
        normed = (message * inv_scale).astype(jnp.bfloat16)
        value = jnp.dot(normed, node_ref[layer], preferred_element_type=jnp.float32)
        return (hidden + value / (1.0 + jnp.exp(-value))).astype(jnp.bfloat16)

    group_rows = (group - 1,) + (group,) * len(ways_y)
    message = jnp.zeros((slots, features), jnp.float32)
    if len(ways_y) > 0:
        landed(places.at[pl.ds(0, group)], pos_recv.at[1])
    tables(0)
    message = gather(0, feats0, 0, message)
    if split:
        landed(places.at[pl.ds(0, group)], pos_recv.at[2])
    tables(1)
    message = gather(0, feats0, 1, message)
    hidden1 = update(0, message, own_hidden)

    def row_of(base, dx, dz):
        return base + (3 * (dx + 1) + dz + 1) * slots

    own_rows = pl.ds(row_of(0, 0, 0), slots)
    feats1[own_rows, :] = hidden1

    def target_base(yo):
        if isinstance(yo, int):
            return 0 if yo == 0 else block
        return jnp.where(group_of(yo) == 2, far_base, block)

    def send_hidden(offs):
        for off in offs:
            row = row_of(target_base(off[1]), off[0], off[2])
            pltpu.make_async_remote_copy(
                src_ref=feats1.at[own_rows],
                dst_ref=feats1.at[pl.ds(pl.multiple_of(row, 16), slots)],
                send_sem=hid_send.at[0],
                recv_sem=hid_recv.at[sem_of(off[1])],
                device_id=target(off),
                device_id_type=MESH,
            ).start()

    if split:
        upper = jnp.where(me[1] == 0, 1, -1)
        last = me[1] == sizes[1] - 1
        to_upper = [(xo, upper, zo) for xo in xd[::-1] for zo in ways_z]
        to_lower = [(xo, -upper, zo) for xo in xd[::-1] for zo in ways_z]
        pl.when(jnp.logical_not(last))(functools.partial(send_hidden, to_upper))
        send_hidden(ring)
        send_hidden(to_lower)
        pl.when(last)(functools.partial(send_hidden, to_upper))
    else:
        for offs in across + [ring]:
            send_hidden(offs)
    sent = len(ring) + sum(len(offs) for offs in across)

    species_row = places[0, 3:4, :]
    offsets = jnp.zeros((1, LANES), jnp.float32)
    for kind in range(kinds):
        offsets = jnp.where(species_row == float(kind), bias_ref[kind], offsets)
    offsets = jnp.where(lane4[0:1] < slots, offsets, 0.0)

    def spread(phase):
        for row, _ in phases[phase][0]:
            base = (0, block, far_base)[row]
            from_base = (0, block, block)[row] if not split else base
            if sizes[1] == 1:
                from_base = 0
            for dx, dz in itertools.product((-1, 0, 1), repeat=2):
                source = row_of(from_base, canonical(dx, sizes[0]), canonical(dz, sizes[2]))
                if source != row_of(base, dx, dz):
                    feats1[pl.ds(row_of(base, dx, dz), slots), :] = feats1[pl.ds(source, slots), :]

    message = jnp.zeros((slots, features), jnp.float32)
    for index, count in enumerate(group_rows[:2]):
        if count:
            landed(feats1.at[pl.ds(0, count * slots)], hid_recv.at[index])
    spread(0)
    message = gather(1, feats1, 0, message)
    if split:
        landed(feats1.at[pl.ds(0, group * slots)], hid_recv.at[2])
    spread(1)
    message = gather(1, feats1, 1, message)
    hidden2 = update(1, message, hidden1.astype(jnp.float32))
    padded = jnp.concatenate(
        [hidden2, jnp.zeros((LANES - slots, features), jnp.bfloat16)], axis=0
    )
    readout = jnp.broadcast_to(readout_ref[...], (16, features))
    per_atom = lax.dot_general(
        readout, padded, (((1,), (1,)), ((), ())), preferred_element_type=jnp.float32
    )
    running = per_atom[0:1, :] + offsets
    energies = running

    def ordered_shifts(axes):
        ys = (
            (side, *range(2, sizes[1] - 1), -side, 0) if split else tuple(range(sizes[1]))[::-1]
        )
        zs = (
            (-far_z, *range(2, sizes[2] - 1), far_z, 0)
            if len(zd) == 3
            else tuple(range(sizes[2]))[::-1]
        )
        xs = tuple(range(sizes[0]))[::-1]
        return [
            (x, y, z)
            for y in (ys if "gy" in axes else (0,))
            for x in (xs if "gx" in axes else (0,))
            for z in (zs if "gz" in axes else (0,))
            if is_set(x) or is_set(y) or is_set(z)
        ]

    for index, (axes, shifts, buf) in enumerate(zip(stages, stage_shifts, stage_bufs)):
        def rank_of(coords):
            rank = 0
            for name, coord, count in zip(AXES, coords, sizes):
                if name in axes:
                    rank = rank * count + coord
            return rank

        mine = rank_of(me)
        buf[mine] = running
        copies = [
            pltpu.make_async_remote_copy(
                src_ref=buf.at[mine],
                dst_ref=buf.at[mine],
                send_sem=red_send.at[index],
                recv_sem=red_recv.at[index],
                device_id=device(shift),
                device_id_type=MESH,
            )
            for shift in ordered_shifts(axes)
        ]
        for copy in copies:
            copy.start()
        if copies:
            landed(buf.at[pl.ds(0, len(copies))], red_recv.at[index])
        running = jnp.sum(buf[...], axis=0)
    out_ref[0:1, :] = energies
    out_ref[1:2, :] = jnp.broadcast_to(jnp.sum(running, axis=1, keepdims=True), (1, LANES))
    if sent:
        landed(places.at[pl.ds(0, sent)], pos_send.at[0])
        landed(feats1.at[pl.ds(0, sent * slots)], hid_send.at[0])
    for index, (shifts, buf) in enumerate(zip(stage_shifts, stage_bufs)):
        if shifts:
            landed(buf.at[pl.ds(0, len(shifts))], red_send.at[index])


def finish(packed, energies, total, energies_here, total_here, sems):
    energies_here[0, 0] = packed[0:1, 0 : energies.shape[-1]]
    total_here[...] = packed[1:2, 0:1]
    first = pltpu.make_async_copy(energies_here, energies, sems.at[0])
    second = pltpu.make_async_copy(total_here, total, sems.at[1])
    first.start()
    second.start()
    first.wait()
    second.wait()


def body(sizes, *args):
    positions, species, neighbours, _, embedding, decay, radial, _, readout, _ = args
    slots = positions.shape[-1]
    features = embedding.shape[1]
    basis_count = decay.shape[0]
    columns = round_up(18 * slots, LANES) + round_up(9 * slots, LANES)
    hi_rows = 16 * pl.cdiv(columns // LANES + 1, 16)
    devices = math.prod(sizes)
    stages = (AXES,) if devices <= 64 else tuple((name,) for name in AXES)
    stage_ranks = [
        math.prod(n for name, n in zip(AXES, sizes) if name in axes) for axes in stages
    ]
    cells = math.prod(len(distinct(n)) for n in sizes)
    vmem = pl.BlockSpec(memory_space=pltpu.VMEM)
    dma = pltpu.SemaphoreType.DMA
    operands = (
        jnp.transpose(positions, (0, 1, 3, 2, 4)),
        *args[1:8],
        readout.reshape(1, features),
        args[9],
    )
    scratch = [
        pltpu.VMEM((cells, 4, LANES), jnp.float32),
        pltpu.VMEM((slots, LANES), jnp.float32),
        pltpu.VMEM((slots * hi_rows, LANES), jnp.float32),
        pltpu.VMEM((slots, neighbours.shape[-1]), jnp.int32),
        pltpu.VMEM((basis_count * slots, columns), jnp.bfloat16),
        pltpu.VMEM((columns, features), jnp.bfloat16),
        pltpu.VMEM((columns, features), jnp.bfloat16),
    ]
    scratch += [
        pltpu.SMEM(x.shape, x.dtype)
        if x.ndim == 1
        else pltpu.VMEM(x.shape, x.dtype)
        for x in operands
    ] + [dma((len(operands),))]
    scratch += [pltpu.VMEM((count, 1, LANES), jnp.float32) for count in stage_ranks]
    scratch += [dma((1,)), dma((3,)), dma((1,)), dma((3,)), dma((len(stages),)), dma((len(stages),))]
    scratch += [pltpu.SemaphoreType.REGULAR]
    out = pl.pallas_call(
        functools.partial(kernel, sizes, stages),
        out_shape=pltpu.VMEM((2, LANES), jnp.float32),
        in_specs=[pl.BlockSpec(memory_space=pl.ANY)] * len(operands),
        out_specs=vmem,
        scratch_shapes=scratch,
        compiler_params=pltpu.CompilerParams(collective_id=0, has_side_effects=True),
    )(*operands)
    anywhere = pl.BlockSpec(memory_space=pl.ANY)
    energies, total = pl.pallas_call(
        finish,
        out_shape=(
            jax.ShapeDtypeStruct(species.shape, jnp.float32),
            jax.ShapeDtypeStruct((1, 1), jnp.float32),
        ),
        in_specs=[vmem],
        out_specs=(anywhere, anywhere),
        scratch_shapes=[
            pltpu.VMEM(species.shape, jnp.float32),
            pltpu.VMEM((1, 1), jnp.float32),
            dma((2,)),
        ],
    )(pltpu.with_memory_space_constraint(out, pltpu.VMEM))
    return energies, total.reshape(())


def solution(mesh):
    sizes = tuple(mesh.shape[name] for name in AXES)
    return jax.shard_map(
        functools.partial(body, sizes),
        mesh=mesh,
        in_specs=(
            P("gx", "gy", "gz", None, None),
            P("gx", "gy", "gz", None),
            P("gx", "gy", "gz", None, None),
            P("gx", "gy", "gz", None),
            P(),
            P(),
            P(),
            P(),
            P(),
            P(),
        ),
        out_specs=(P("gx", "gy", "gz", None), P()),
        check_vma=False,
    )
```

```python
import functools
import itertools
import math

import jax
import jax.numpy as jnp
from jax import lax
from jax.experimental import pallas as pl
from jax.experimental.pallas import tpu as pltpu
from jax.sharding import PartitionSpec as P

AXES = ("gx", "gy", "gz")
MESH = pl.DeviceIdType.MESH
LANES = 128
LOG2E = math.log2(math.e)


def distinct(count):
    return (0,) if count == 1 else (0, -1) if count == 2 else (0, -1, 1)


def canonical(offset, count):
    return 0 if count == 1 else -abs(offset) if count == 2 else offset


def is_set(offset):
    return not isinstance(offset, int) or offset != 0


def as_int(flag):
    return int(flag) if isinstance(flag, bool) else flag.astype(jnp.int32)


def round_up(value, unit):
    return -(-value // unit) * unit


def reach(sizes, steps):
    found = {(0, 0, 0)}
    for _ in range(steps):
        found = {
            tuple((a + b) % n for a, b, n in zip(shift, off, sizes))
            for shift in found
            for off in itertools.product((-1, 0, 1), repeat=3)
        }
    return found


def kernel(
    sizes,
    stages,
    pos_any,
    spec_any,
    nbr_any,
    cnt_any,
    emb_any,
    decay_any,
    radial_any,
    node_any,
    readout_any,
    bias_any,
    out_ref,
    places,
    cols,
    hist,
    codes,
    basis,
    feats0,
    feats1,
    *rest,
):
    anys = (
        pos_any, spec_any, nbr_any, cnt_any, emb_any, decay_any, radial_any, node_any, readout_any, bias_any,
    )
    pos_ref, spec_ref, nbr_ref, cnt_ref, emb_ref = rest[:5]
    decay_ref, radial_ref, node_ref, readout_ref, bias_ref = rest[5:10]
    local = rest[:10]
    load_sem = rest[10]
    rest = rest[11:]
    stage_bufs = rest[: len(stages)]
    pos_send, pos_recv, hid_send, hid_recv, red_send, red_recv, entered = rest[len(stages) :]
    me = tuple(lax.axis_index(name) for name in AXES)
    slots = pos_any.shape[-1]
    neighbour_count = nbr_any.shape[-1]
    features = emb_any.shape[1]
    kinds = emb_any.shape[0]
    basis_count = radial_ref.shape[1]
    hi_rows = hist.shape[0] // slots
    block = 9 * slots
    far_base = round_up(2 * block, LANES)
    columns = basis.shape[1]
    xd, yd, zd = (distinct(n) for n in sizes)
    group = len(xd) * len(zd)
    split = len(yd) == 3

    loads = [
        pltpu.make_async_copy(src, dst, load_sem.at[n])
        for n, (src, dst) in enumerate(zip(anys, local))
    ]
    for n in (0, 1, 3, 2, 4, 5, 6, 7, 8, 9):
        loads[n].start()

    def wrapped(coord, delta, count):
        if isinstance(delta, int):
            return lax.rem(coord + (delta % count), count) if delta % count else coord
        return lax.rem(coord + delta + count, count)

    def device(shift):
        return tuple(wrapped(c, d, n) for c, d, n in zip(me, shift, sizes))

    def last_offset(coord):
        return jnp.where(2 * coord < sizes[1], -1, 1)

    side = last_offset(me[1])

    stage_shifts = [
        [
            shift
            for shift in itertools.product(
                *(range(n) if name in axes else (0,) for name, n in zip(AXES, sizes))
            )
            if any(shift)
        ]
        for axes in stages
    ]
    def landed(ref, sem):
        pltpu.make_async_copy(ref, ref, sem).wait()

    far_z = jnp.where(lax.rem(me[2], 2) == 0, 1, -1) if len(zd) == 3 else zd[-1]
    ways_z = (far_z, -far_z, 0) if len(zd) == 3 else zd[::-1]
    ways_y = (-side, side) if split else yd[1:]

    def target(off):
        return tuple(wrapped(c, -d, n) for c, d, n in zip(me, off, sizes))

    ring = [(xo, 0, zo) for xo in xd[::-1] for zo in ways_z if is_set(xo) or is_set(zo)]
    across = [[(xo, yo, zo) for xo in xd[::-1] for zo in ways_z] for yo in ways_y]

    sent = len(ring) + sum(len(offs) for offs in across)

    def wrap_of(yo):
        to = wrapped(me[1], -yo, sizes[1])
        return to - me[1] > 1, me[1] - to > 1

    known = reach(sizes, 2)
    others = sorted({s for shifts in stage_shifts for s in shifts if s not in known})
    barrier = pltpu.get_barrier_semaphore()

    for shift in others:
        pl.semaphore_signal(barrier, inc=1, device_id=device(shift), device_id_type=MESH)
    def greet(offs):
        for off in offs:
            pl.semaphore_signal(barrier, inc=1, device_id=target(off), device_id_type=MESH)

    greet(ring)
    greeted = len(ring) + len(others)
    for offs in across:
        low, high = wrap_of(offs[0][1])
        pl.when(jnp.logical_not(high))(functools.partial(greet, offs))
        greeted += len(offs) * (1 - as_int(low))

    def group_of(yo):
        if not is_set(yo) or not split:
            return 0 if yo == 0 else 1
        return jnp.where(yo == last_offset(wrapped(me[1], -yo, sizes[1])), 2, 1)

    def sem_of(yo):
        return group_of(yo)

    loads[0].wait()
    loads[1].wait()
    places[0] = jnp.zeros(places.shape[1:], jnp.float32)
    places[0, 0:3, 0:slots] = pos_ref[0, 0, :, 0]
    places[0, 3:4, 0:slots] = spec_ref[0, 0].astype(jnp.float32)

    def prepare():
        loads[3].wait()
        counts = jnp.concatenate(
            [cnt_ref[0, 0].astype(jnp.float32), jnp.zeros((1, LANES - slots), jnp.float32)], axis=1
        )
        turned = jnp.transpose(
            jnp.concatenate([places[0], counts, jnp.zeros((3, LANES), jnp.float32)], axis=0)
        )[0:slots]
        cols[:, 0:8] = turned
        count_col = turned[:, 4:5]
        loads[2].wait()
        raw = nbr_ref[0, 0, 0]
        live = lax.broadcasted_iota(jnp.int32, raw.shape, 1).astype(jnp.float32) < count_col
        x_step = jnp.where(raw >= 2 * block, 2, jnp.where(raw >= block, 1, 0))
        inner = raw - x_step * block
        y_low = inner < 3 * slots
        y_high = inner >= 6 * slots
        depth = inner - jnp.where(y_low, 0, jnp.where(y_high, 6 * slots, 3 * slots))
        low_base = jnp.where(side < 0, far_base, block)
        high_base = jnp.where(side < 0, block, far_base)
        place = depth + x_step * (3 * slots) + jnp.where(
            y_low, low_base, jnp.where(y_high, high_base, 0)
        )
        codes[...] = jnp.where(live, place, hi_rows * LANES - 1)
        hi_iota = lax.broadcasted_iota(jnp.int32, (hi_rows, neighbour_count), 0)
        lo_iota = lax.broadcasted_iota(jnp.int32, (LANES, neighbour_count), 0)
        for atom in range(slots):
            row = codes[atom : atom + 1, :]
            high = jnp.where((row >> 7) == hi_iota, 1.0, 0.0).astype(jnp.bfloat16)
            low = jnp.where((row & (LANES - 1)) == lo_iota, 1.0, 0.0).astype(jnp.bfloat16)
            hist[atom * hi_rows : (atom + 1) * hi_rows, :] = lax.dot_general(
                high, low, (((1,), (1,)), ((), ())), preferred_element_type=jnp.float32
            )

    def slot_of(xo, yo, zo):
        z = zd.index(zo) if isinstance(zo, int) else jnp.where(zo < 0, 1, 2)
        return group_of(yo) * group + xd.index(xo) * len(zd) + z

    def send_place(off):
        pltpu.make_async_remote_copy(
            src_ref=places.at[0],
            dst_ref=places.at[slot_of(*off)],
            send_sem=pos_send.at[0],
            recv_sem=pos_recv.at[sem_of(off[1])],
            device_id=target(off),
            device_id_type=MESH,
        ).start()

    pl.semaphore_wait(barrier, greeted)
    for offs in across:
        low, high = wrap_of(offs[0][1])

        @pl.when(high)
        def _():
            pl.semaphore_signal(
                entered, inc=1, device_id=target((0, offs[0][1], 0)), device_id_type=MESH
            )

    def send_ring():
        for off in ring:
            send_place(off)

    first_plane = me[1] == 0
    pl.when(first_plane)(send_ring)
    for offs in across:
        low, high = wrap_of(offs[0][1])

        @pl.when(jnp.logical_not(low))
        def _():
            for off in offs:
                send_place(off)

    pl.when(jnp.logical_not(first_plane))(send_ring)

    prepare()

    if group > 1:
        landed(places.at[pl.ds(0, group - 1)], pos_recv.at[0])
    for offs in across:
        low, high = wrap_of(offs[0][1])

        @pl.when(low)
        def _():
            yo = offs[0][1]
            pl.semaphore_wait(entered, 1)
            pltpu.make_async_remote_copy(
                src_ref=places.at[pl.ds(0, group)],
                dst_ref=places.at[pl.ds(group_of(yo) * group, group)],
                send_sem=pos_send.at[0],
                recv_sem=pos_recv.at[sem_of(yo)],
                device_id=target((0, yo, 0)),
                device_id_type=MESH,
            ).start()

    for n in range(4, 10):
        loads[n].wait()
    near_rows = slice(2 * block, far_base)
    far_rows = slice(far_base + block, columns)
    for span in (near_rows, far_rows):
        if span.stop > span.start:
            feats1[span, :] = jnp.zeros((span.stop - span.start, features), jnp.bfloat16)
    own_pos = [jnp.broadcast_to(cols[:, c : c + 1], (slots, LANES)) for c in range(3)]
    species_col = cols[:, 3:4]
    own_hidden = jnp.zeros((slots, features), jnp.float32)
    for kind in range(kinds):
        own_hidden = jnp.where(
            species_col == float(kind), emb_ref[kind : kind + 1, :].astype(jnp.float32), own_hidden
        )
    emb = emb_ref[...].astype(jnp.float32)
    if kinds < 8:
        emb = jnp.concatenate([emb, jnp.zeros((8 - kinds, features), jnp.float32)], axis=0)
    emb = emb.astype(jnp.bfloat16)
    scales = [decay_ref[b] * (-LOG2E) for b in range(basis_count)]
    lane4 = lax.broadcasted_iota(jnp.int32, (4, LANES), 1)
    sub4 = lax.broadcasted_iota(jnp.int32, (4, LANES), 0)
    sub = lax.broadcasted_iota(jnp.int32, (8, LANES), 0)

    plane_stop = block // LANES * LANES
    cells = [
        (row, dy, dx, dz, (far_base if row == 2 else row * block) + index * slots)
        for row, dy in ((0, 0), (1, -side), (2, side))
        for index, (dx, dz) in enumerate(itertools.product((-1, 0, 1), repeat=2))
    ]
    phases = (
        ((0, far_base), (far_base, columns)),
        ((0, plane_stop), (plane_stop, far_base), (far_base, columns)),
    )

    def source_slot(row, dx, dz):
        if not split:
            row = 0 if row == 0 or sizes[1] == 1 else 1
        x = xd.index(canonical(dx, sizes[0]))
        z = zd.index(canonical(dz, sizes[2]))
        return row * group + x * len(zd) + z

    def tables(phase):
        first, stop = phases[0][phase]
        flat = [jnp.zeros((4, LANES), jnp.float32) for _ in range((stop - first) // LANES)]
        for row, dy, dx, dz, column in cells:
            if column + slots <= first or column >= stop:
                continue
            cell = places[source_slot(row, dx, dz)]
            delta = jnp.zeros((4, LANES), jnp.float32)
            if dx:
                delta = jnp.where(sub4 == 0, float(dx), delta)
            if row:
                delta = jnp.where(sub4 == 1, jnp.asarray(dy, jnp.float32), delta)
            if dz:
                delta = jnp.where(sub4 == 2, float(dz), delta)
            if dx or row or dz:
                cell = cell + delta
            tile, start = divmod(column - first, LANES)
            if start:
                cell = pltpu.roll(cell, start, 1)
            end = start + slots
            if tile >= 0:
                flat[tile] = jnp.where((lane4 >= start) & (lane4 < end), cell, flat[tile])
            if end > LANES and tile + 1 < len(flat):
                flat[tile + 1] = jnp.where(lane4 < end - LANES, cell, flat[tile + 1])
        for index, table in enumerate(flat):
            span = slice(first + index * LANES, first + (index + 1) * LANES)
            r2 = jnp.zeros((slots, LANES), jnp.float32)
            for c in range(3):
                delta = table[c : c + 1, :] - own_pos[c]
                r2 = r2 + delta * delta
            times = hist[pl.ds(first // LANES + index, slots, stride=hi_rows), :]
            for b in range(basis_count):
                basis[b * slots : (b + 1) * slots, span] = (
                    jnp.exp2(r2 * scales[b]) * times
                ).astype(jnp.bfloat16)
            one_hot = jnp.where(table[3:4, :].astype(jnp.int32) == sub, 1.0, 0.0)
            feats0[span, :] = jnp.dot(
                jnp.transpose(one_hot).astype(jnp.bfloat16), emb, preferred_element_type=jnp.float32
            ).astype(jnp.bfloat16)

    def gather(layer, feats, phase, message):
        first, stop = phases[layer][phase]
        weight = radial_ref[layer].astype(jnp.float32)
        step = basis_count // 4
        for lead_b in range(0, basis_count, step):
            collected = jnp.dot(
                basis[lead_b * slots : (lead_b + step) * slots, first:stop],
                feats[first:stop, :],
                preferred_element_type=jnp.float32,
            )
            for b in range(step):
                message = message + (
                    collected[b * slots : (b + 1) * slots] * weight[lead_b + b : lead_b + b + 1]
                )
        return message

    def update(layer, message, hidden):
        inv_scale = lax.rsqrt(jnp.mean(message * message, axis=-1, keepdims=True) + 1e-05)
        normed = (message * inv_scale).astype(jnp.bfloat16)
        value = jnp.dot(normed, node_ref[layer], preferred_element_type=jnp.float32)
        return (hidden + value / (1.0 + jnp.exp(-value))).astype(jnp.bfloat16)

    group_rows = (group - 1,) + (group,) * len(ways_y)
    message = jnp.zeros((slots, features), jnp.float32)
    for phase in range(2):
        if phase < len(ways_y):
            landed(places.at[pl.ds(0, group)], pos_recv.at[phase + 1])
        tables(phase)
        message = gather(0, feats0, phase, message)
    hidden1 = update(0, message, own_hidden)

    def row_of(base, dx, dz):
        return base + (3 * (dx + 1) + dz + 1) * slots

    own_rows = pl.ds(row_of(0, 0, 0), slots)
    feats1[own_rows, :] = hidden1

    def target_base(yo):
        if not is_set(yo) or not split:
            return 0 if yo == 0 else block
        return jnp.where(group_of(yo) == 2, far_base, block)

    def target_base_here(yo):
        return jnp.where(side == yo, far_base, block)

    def send_hidden(offs, out_sem, in_sem=None):
        for off in offs:
            row = row_of(target_base(off[1]), off[0], off[2])
            pltpu.make_async_remote_copy(
                src_ref=feats1.at[own_rows],
                dst_ref=feats1.at[pl.ds(pl.multiple_of(row, 16), slots)],
                send_sem=hid_send.at[out_sem],
                recv_sem=hid_recv.at[sem_of(off[1]) if in_sem is None else in_sem],
                device_id=target(off),
                device_id_type=MESH,
            ).start()

    shared = split and len(zd) == 3 and sizes[2] % 2 == 0
    odd = lax.rem(me[2], 2) == 1
    last_plane = me[1] == sizes[1] - 1
    inner_plane = jnp.logical_not(jnp.logical_or(first_plane, last_plane))
    up = [(xo, -1, zo) for xo in xd[::-1] for zo in ways_z]
    down = [(xo, 1, zo) for xo in xd[::-1] for zo in ways_z]
    handed = 2 * len(xd)
    hands_on = jnp.logical_and(odd, jnp.logical_not(first_plane))

    def send_up():
        if not shared:
            send_hidden(up, 1)
            return
        send_hidden([(xo, -1, jnp.where(odd, 0, -1)) for xo in xd[::-1]], 1, 3)
        send_hidden([(xo, -1, far_z) for xo in xd[::-1]], 1)

    if split:
        pl.when(first_plane)(functools.partial(send_hidden, down, 0))
        pl.when(inner_plane)(send_up)
        send_hidden(ring, 0)
        pl.when(first_plane)(send_up)
        pl.when(jnp.logical_not(first_plane))(functools.partial(send_hidden, down, 0))
        pl.when(last_plane)(functools.partial(send_hidden, up, 1))
    else:
        for offs in across + [ring]:
            send_hidden(offs, 0)
    if shared:
        base = target_base_here(-1)

        @pl.when(hands_on)
        def _():
            landed(feats1.at[pl.ds(0, handed * slots)], hid_recv.at[3])
            for xo in xd[::-1]:
                rows = [
                    pl.ds(pl.multiple_of(row_of(base, xo, dz), 16), 2 * slots) for dz in (-1, 0)
                ]
                pltpu.make_async_remote_copy(
                    src_ref=feats1.at[rows[0]],
                    dst_ref=feats1.at[rows[1]],
                    send_sem=hid_send.at[2],
                    recv_sem=hid_recv.at[jnp.where(side < 0, 2, 1)],
                    device_id=target((0, 0, 1)),
                    device_id_type=MESH,
                ).start()

    species_row = places[0, 3:4, :]
    offsets = jnp.zeros((1, LANES), jnp.float32)
    for kind in range(kinds):
        offsets = jnp.where(species_row == float(kind), bias_ref[kind], offsets)
    offsets = jnp.where(lane4[0:1] < slots, offsets, 0.0)

    def spread(row):
        base = (0, block, far_base)[row]
        from_base = base if split else 0 if row == 0 or sizes[1] == 1 else block
        for dx, dz in itertools.product((-1, 0, 1), repeat=2):
            source = row_of(from_base, canonical(dx, sizes[0]), canonical(dz, sizes[2]))
            if source != row_of(base, dx, dz):
                feats1[pl.ds(row_of(base, dx, dz), slots), :] = feats1[pl.ds(source, slots), :]

    message = jnp.zeros((slots, features), jnp.float32)
    for phase in range(3):
        if phase <= len(ways_y) and group_rows[phase]:
            whole = feats1.at[pl.ds(0, group_rows[phase] * slots)]
            if shared and phase:
                below = side == -1 if phase == 2 else side == 1
                part = jnp.logical_and(hands_on, below)
                rest_rows = feats1.at[pl.ds(0, (group_rows[phase] - handed) * slots)]
                pl.when(part)(functools.partial(landed, rest_rows, hid_recv.at[phase]))
                pl.when(jnp.logical_not(part))(
                    functools.partial(landed, whole, hid_recv.at[phase])
                )
            else:
                landed(whole, hid_recv.at[phase])
        spread(phase)
        message = gather(1, feats1, phase, message)
    hidden2 = update(1, message, hidden1.astype(jnp.float32))
    readout_row = readout_ref[...].astype(jnp.float32)
    running = jnp.sum(hidden2.astype(jnp.float32) * readout_row, axis=0, keepdims=True) + offsets

    def ordered_shifts(axes):
        ys = (
            (side, *range(2, sizes[1] - 1), -side, 0) if split else tuple(range(sizes[1]))[::-1]
        )
        zs = (
            (-far_z, *range(2, sizes[2] - 1), far_z, 0)
            if len(zd) == 3
            else tuple(range(sizes[2]))[::-1]
        )
        xs = tuple(range(sizes[0]))[::-1]
        return [
            (x, y, z)
            for y in (ys if "gy" in axes else (0,))
            for x in (xs if "gx" in axes else (0,))
            for z in (zs if "gz" in axes else (0,))
            if is_set(x) or is_set(y) or is_set(z)
        ]

    for index, (axes, shifts, buf) in enumerate(zip(stages, stage_shifts, stage_bufs)):
        def rank_of(coords):
            rank = 0
            for name, coord, count in zip(AXES, coords, sizes):
                if name in axes:
                    rank = rank * count + coord
            return rank

        mine = rank_of(me)
        buf[mine] = running
        copies = [
            pltpu.make_async_remote_copy(
                src_ref=buf.at[mine],
                dst_ref=buf.at[mine],
                send_sem=red_send.at[index],
                recv_sem=red_recv.at[index],
                device_id=device(shift),
                device_id_type=MESH,
            )
            for shift in ordered_shifts(axes)
        ]
        for copy in copies:
            copy.start()
        if index == 0:
            padded = jnp.concatenate(
                [hidden2, jnp.zeros((LANES - slots, features), jnp.bfloat16)], axis=0
            )
            per_atom = lax.dot_general(
                jnp.broadcast_to(readout_ref[...], (16, features)),
                padded,
                (((1,), (1,)), ((), ())),
                preferred_element_type=jnp.float32,
            )
            out_ref[0:1, :] = per_atom[0:1, :] + offsets
        if copies:
            landed(buf.at[pl.ds(0, len(copies))], red_recv.at[index])
        running = jnp.sum(buf[...], axis=0)
    out_ref[1:2, :] = jnp.broadcast_to(jnp.sum(running, axis=1, keepdims=True), (1, LANES))
    if sent:
        landed(places.at[pl.ds(0, sent)], pos_send.at[0])
        later = len(up) if split else 0
        landed(feats1.at[pl.ds(0, (sent - later) * slots)], hid_send.at[0])
    if split:
        fewer = len(up) - handed + len(xd) if shared else len(up)

        def drain(flag, count, index):
            pl.when(flag)(
                functools.partial(landed, feats1.at[pl.ds(0, count * slots)], hid_send.at[index])
            )

        drain(last_plane, len(up), 1)
        drain(jnp.logical_not(last_plane), fewer, 1)
        if shared:
            drain(hands_on, handed, 2)
    for index, (shifts, buf) in enumerate(zip(stage_shifts, stage_bufs)):
        if shifts:
            landed(buf.at[pl.ds(0, len(shifts))], red_send.at[index])


def finish(packed, energies, total, energies_here, total_here, sems):
    energies_here[0, 0] = packed[0:1, 0 : energies.shape[-1]]
    total_here[...] = packed[1:2, 0:1]
    first = pltpu.make_async_copy(energies_here, energies, sems.at[0])
    second = pltpu.make_async_copy(total_here, total, sems.at[1])
    first.start()
    second.start()
    first.wait()
    second.wait()


def body(sizes, *args):
    positions, species, neighbours, _, embedding, decay, radial, _, readout, _ = args
    slots = positions.shape[-1]
    features = embedding.shape[1]
    basis_count = decay.shape[0]
    columns = round_up(18 * slots, LANES) + round_up(9 * slots, LANES)
    hi_rows = 16 * pl.cdiv(columns // LANES + 1, 16)
    devices = math.prod(sizes)
    stages = (AXES,) if devices <= 64 else tuple((name,) for name in AXES)
    stage_ranks = [
        math.prod(n for name, n in zip(AXES, sizes) if name in axes) for axes in stages
    ]
    cells = math.prod(len(distinct(n)) for n in sizes)
    vmem = pl.BlockSpec(memory_space=pltpu.VMEM)
    dma = pltpu.SemaphoreType.DMA
    operands = (
        jnp.transpose(positions, (0, 1, 3, 2, 4)),
        *args[1:8],
        readout.reshape(1, features),
        args[9],
    )
    scratch = [
        pltpu.VMEM((cells, 4, LANES), jnp.float32),
        pltpu.VMEM((slots, LANES), jnp.float32),
        pltpu.VMEM((slots * hi_rows, LANES), jnp.float32),
        pltpu.VMEM((slots, neighbours.shape[-1]), jnp.int32),
        pltpu.VMEM((basis_count * slots, columns), jnp.bfloat16),
        pltpu.VMEM((columns, features), jnp.bfloat16),
        pltpu.VMEM((columns, features), jnp.bfloat16),
    ]
    scratch += [
        pltpu.SMEM(x.shape, x.dtype)
        if x.ndim == 1
        else pltpu.VMEM(x.shape, x.dtype)
        for x in operands
    ] + [dma((len(operands),))]
    scratch += [pltpu.VMEM((count, 1, LANES), jnp.float32) for count in stage_ranks]
    scratch += [dma((1,)), dma((3,)), dma((3,)), dma((4,)), dma((len(stages),)), dma((len(stages),))]
    scratch += [pltpu.SemaphoreType.REGULAR]
    out = pl.pallas_call(
        functools.partial(kernel, sizes, stages),
        out_shape=pltpu.VMEM((2, LANES), jnp.float32),
        in_specs=[pl.BlockSpec(memory_space=pl.ANY)] * len(operands),
        out_specs=vmem,
        scratch_shapes=scratch,
        compiler_params=pltpu.CompilerParams(collective_id=0, has_side_effects=True),
    )(*operands)
    anywhere = pl.BlockSpec(memory_space=pl.ANY)
    energies, total = pl.pallas_call(
        finish,
        out_shape=(
            jax.ShapeDtypeStruct(species.shape, jnp.float32),
            jax.ShapeDtypeStruct((1, 1), jnp.float32),
        ),
        in_specs=[vmem],
        out_specs=(anywhere, anywhere),
        scratch_shapes=[
            pltpu.VMEM(species.shape, jnp.float32),
            pltpu.VMEM((1, 1), jnp.float32),
            dma((2,)),
        ],
    )(pltpu.with_memory_space_constraint(out, pltpu.VMEM))
    return energies, total.reshape(())


def solution(mesh):
    sizes = tuple(mesh.shape[name] for name in AXES)
    return jax.shard_map(
        functools.partial(body, sizes),
        mesh=mesh,
        in_specs=(
            P("gx", "gy", "gz", None, None),
            P("gx", "gy", "gz", None),
            P("gx", "gy", "gz", None, None),
            P("gx", "gy", "gz", None),
            P(),
            P(),
            P(),
            P(),
            P(),
            P(),
        ),
        out_specs=(P("gx", "gy", "gz", None), P()),
        check_vma=False,
    )
```
